32 devices in a mesh: mp: 8 (over y, x, core), hidden: 4 (over z).
Axes of the slice: x: 2, y: 2, z: 4, core: 2. Of those that a mesh axis runs over, the one named last changes fastest.
Arguments:
- states: bfloat16 [512, 16384], P(None, 'mp'), may hold values from -6 to 6
- gate_codes: bfloat16 [16384, 26624], P('mp', 'hidden'), may hold values from -127 to 127, as said below
- gate_scales: float32 [128, 26624], P('mp', 'hidden'), may hold values from 7.8125e-05 to 0.000703125
- up_codes: bfloat16 [16384, 26624], P('mp', 'hidden'), may hold values from -127 to 127, as said below
- up_scales: float32 [128, 26624], P('mp', 'hidden'), may hold values from 7.8125e-05 to 0.000703125
- down_codes: bfloat16 [26624, 16384], P('hidden', 'mp'), may hold values from -127 to 127, as said below
- down_scales: float32 [208, 16384], P('hidden', 'mp'), may hold values from 1.2257258e-05 to 0.000110315326
Outputs:
- output: bfloat16 [512, 16384], P(None, 'mp')
The draws below stay inside these ranges and needn't reach their ends.
Inputs may be any that keep to these rules, and one draw needn't show every extreme that they name: `gate_codes`: whole numbers. `up_codes`: whole numbers. `down_codes`: whole numbers.
All inputs are finite; a program needn't handle non-finite values. Where the reference program divides by a largest or mean magnitude, that divisor is 1e-20 or more.
Results may differ from the reference program's by a relative error of at most 0.02.
Values may be sent and summed in bfloat16 or wider, within the bound.
A program may use at most 256 MiB of HBM per device.

```python
import math
import jax
import jax.numpy as jnp

D = 16384
FF = 26624
BLOCK = 128
ROWS = 512
N_MP = 8
N_HIDDEN = 4


def draw_gate_codes(key, part):
    return jax.random.randint(jax.random.fold_in(key, 11), (D, FF), -127, 128).astype(jnp.float32).astype(jnp.bfloat16)


def draw_up_codes(key, part):
    return jax.random.randint(jax.random.fold_in(key, 23), (D, FF), -127, 128).astype(jnp.float32).astype(jnp.bfloat16)


def draw_down_codes(key, part):
    return jax.random.randint(jax.random.fold_in(key, 37), (FF, D), -127, 128).astype(jnp.float32).astype(jnp.bfloat16)


def steps_of(own_key, extent, shards, low, high):
    loudness, own = 1.0, jax.random.fold_in(own_key, 6)
    for dim, shards_of in shards:
        heights = jnp.exp(jax.random.uniform(jax.random.fold_in(own, dim), (shards_of,), jnp.float32, low / len(shards), high / len(shards)))
        loudness = loudness * jnp.repeat(heights, extent[dim] // shards_of).reshape([-1 if axis == dim else 1 for axis in range(len(extent))])
    return loudness


def centred(rng, dims, deviation, most, split=(), held_as=jnp.bfloat16):
    values = deviation * jax.random.normal(rng, dims, jnp.float32)
    if split:
        values = values * steps_of(rng, dims, split, -0.22, 0.18)
    return jnp.clip(values, -most, most).astype(held_as)


def setup_inputs(seed: int = 0) -> dict:
    arg_keys = jax.random.split(jax.random.key(seed), 8)
    states = centred(arg_keys[0], (ROWS, D), 1.0, 6.0, ((1, 8),))
    gate_codes = draw_gate_codes(jax.random.fold_in(arg_keys[7], 71), 0)
    gate_scales = jnp.clip(jnp.exp(math.log(0.000703125) - 2.1972246 * jax.random.uniform(arg_keys[2], (D // BLOCK, FF), jnp.float32) ** steps_of(arg_keys[2], (D // BLOCK, FF), ((0, 8), (1, 4)), -0.2, 0.2)), 7.812499825377017e-05, 0.000703125)
    up_codes = draw_up_codes(jax.random.fold_in(arg_keys[7], 71), 0)
    up_scales = jnp.clip(jnp.exp(math.log(0.000703125) - 2.1972246 * jax.random.uniform(arg_keys[4], (D // BLOCK, FF), jnp.float32) ** steps_of(arg_keys[4], (D // BLOCK, FF), ((0, 8), (1, 4)), -0.2, 0.2)), 7.812499825377017e-05, 0.000703125)
    down_codes = draw_down_codes(jax.random.fold_in(arg_keys[7], 71), 0)
    down_scales = jnp.clip(jnp.exp(math.log(0.000110315326) - 2.1972246 * jax.random.uniform(arg_keys[6], (FF // BLOCK, D), jnp.float32) ** steps_of(arg_keys[6], (FF // BLOCK, D), ((0, 4), (1, 8)), -0.2, 0.2)), 1.225725827680435e-05, 0.000110315326)
    return dict(states=states, gate_codes=gate_codes, gate_scales=gate_scales, up_codes=up_codes, up_scales=up_scales, down_codes=down_codes, down_scales=down_scales)


epsilon = 1e-6


def dequantize(quantized, scales):
    depth, columns = quantized.shape
    groups = scales.shape[0]
    blocks = quantized.astype(jnp.float32).reshape(groups, depth // groups, columns)
    return (blocks * scales.astype(jnp.float32)[:, None, :]).reshape(depth, columns).astype(jnp.bfloat16)


def encode(values):
    row_count, columns = values.shape
    blocks = values.reshape(row_count, columns // BLOCK, BLOCK)
    maxima = (jnp.max(jnp.abs(blocks), axis=-1) + epsilon).astype(jnp.bfloat16)
    factor = 127.0 / maxima.astype(jnp.float32)
    codes = (blocks * factor[..., None]).astype(jnp.bfloat16)
    return codes.reshape(row_count, columns), maxima


def decode(codes, maxima):
    row_count, columns = codes.shape
    blocks = codes.astype(jnp.float32).reshape(row_count, columns // BLOCK, BLOCK)
    step_size = maxima.astype(jnp.float32) / 127.0
    return (blocks * step_size[..., None]).reshape(row_count, columns)


def reference(states, gate_codes, gate_scales, up_codes, up_scales, down_codes, down_scales):
    piece = D // N_MP
    groups = piece // BLOCK
    gate_sum = jnp.zeros((ROWS, FF), jnp.float32)
    up_sum = jnp.zeros((ROWS, FF), jnp.float32)
    for source in range(N_MP):
        inputs = states[:, source * piece:(source + 1) * piece]
        gate_w = dequantize(gate_codes[source * piece:(source + 1) * piece], gate_scales[source * groups:(source + 1) * groups])
        gate_part = jnp.dot(inputs, gate_w, preferred_element_type=jnp.float32)
        gate_sum = gate_sum + decode(*encode(gate_part))
        up_w = dequantize(up_codes[source * piece:(source + 1) * piece], up_scales[source * groups:(source + 1) * groups])
        up_part = jnp.dot(inputs, up_w, preferred_element_type=jnp.float32)
        up_sum = up_sum + decode(*encode(up_part))
    swiglu = jax.nn.silu(gate_sum) * up_sum
    activation = decode(*encode(swiglu)).astype(jnp.bfloat16)
    width = FF // N_HIDDEN
    wgroups = width // BLOCK
    result = jnp.zeros((ROWS, D), jnp.float32)
    for owner in range(N_HIDDEN):
        down_w = dequantize(down_codes[owner * width:(owner + 1) * width], down_scales[owner * wgroups:(owner + 1) * wgroups])
        result = result + jnp.dot(activation[:, owner * width:(owner + 1) * width], down_w, preferred_element_type=jnp.float32)
    return (result + states.astype(jnp.float32)).astype(jnp.bfloat16)
```

```python
import functools

import jax
import jax.numpy as jnp
from jax import lax
from jax.experimental import pallas as pl
from jax.experimental.pallas import tpu as pltpu
from jax.sharding import PartitionSpec as P

F32, BF16 = jnp.float32, jnp.bfloat16
MESH = pl.DeviceIdType.MESH
SPLITS = 2
SLOTS = 4


def dequant(codes, scales):
    depth, columns = codes.shape
    groups = scales.shape[0]
    blocks = codes.astype(F32).reshape(groups, depth // groups, columns)
    return (blocks * scales.reshape(groups, 1, columns)).reshape(depth, columns).astype(BF16)


class Plan:
    def __init__(self, n, nz, rows, depth, hidden):
        self.n, self.nz, self.depth, self.hidden = n, nz, depth, hidden
        self.nb = n.bit_length() - 1
        self.h = SPLITS
        self.rb = rows // n // SPLITS
        self.w = next(t for t in (512, 256) if hidden % t == 0)
        self.wq = self.w // 2
        self.c = hidden // self.w
        self.u = self.c * self.h
        self.j = depth // self.wq
        self.v = self.j * self.h
        self.k2 = hidden // 2
        self.wrows = max(2 * depth, self.k2)
        dims = list(range(self.nb))
        self.orders = (dims, dims[:1] + dims[:0:-1])
        self.mid = nz // 2

    def left(self, q, k):
        return sorted(set(range(self.nb)) - set(self.orders[q][: k + 1]))

    def mask(self, pos):
        return sum(((pos >> (self.nb - 1 - d)) & 1) << d for d in range(self.nb))


def kernel(p, x_hbm, gc, uc, dc, gs, us, ds, out, xp, w, ps, r0, rk, act, zs, zr, zx, zf, sems):
    n, nb, C, U, J, V, rb, wq = p.n, p.nb, p.c, p.u, p.j, p.v, p.rb, p.wq
    me = lax.axis_index("mp").astype(jnp.int32)
    z = lax.axis_index("hidden").astype(jnp.int32)
    nz = p.nz
    on_left = z < p.mid
    deep = jnp.where(on_left, z, nz - 1 - z)
    inward = jnp.where(on_left, z + 1, z - 1)
    outward = jnp.where(on_left, z - 1, z + 1)
    every = slice(None)

    def index(fixed, dims):
        return tuple(fixed.get(d, every) for d in dims)

    def x_copy(h, pos):
        return pltpu.make_async_copy(x_hbm.at[me ^ p.mask(pos), h], xp.at[h, pos], sems["x"].at[h * n + pos])

    def w_copy(c, i):
        slot = lax.rem(c, 2)
        columns = pl.ds(pl.multiple_of(c * p.w, p.w), p.w)
        return pltpu.make_async_copy(
            (gc, uc)[i].at[:, columns], w.at[slot, pl.ds(i * p.depth, p.depth)], sems["w"].at[slot, i]
        )

    def d_copy(v, i):
        slot = lax.rem(v, 2)
        columns = pl.ds(pl.multiple_of(lax.rem(v, J) * wq, wq), wq)
        return pltpu.make_async_copy(
            dc.at[pl.ds(i * p.k2, p.k2), columns],
            w.at[slot, pl.ds(0, p.k2), pl.ds(i * wq, wq)],
            sems["w"].at[slot, i],
        )

    def remote(src, dst, send, recv, to):
        return pltpu.make_async_remote_copy(
            src_ref=src, dst_ref=dst, send_sem=send, recv_sem=recv, device_id=to, device_id_type=MESH
        )

    def part_at(u, q, fixed):
        return (u,) + index(fixed, range(nb)) + (q,)

    def sum_copy(s, q):
        d = p.orders[q][s]

        def make(u):
            slot = lax.rem(u, SLOTS)
            to = (me ^ (1 << d), z)
            if s == 0:
                return remote(ps.at[u, 1], r0.at[u], sems["s0"].at[slot], sems["r0"].at[u], to)
            fixed = {e: 0 for e in p.orders[q][:s]} | {d: 1}
            return remote(
                ps.at[part_at(u, q, fixed)],
                rk[s - 1].at[u, q],
                sems["sk"].at[s - 1, q, slot],
                sems["rk"].at[s - 1, q, u],
                to,
            )

        return make

    def act_copy(k, q):
        d = p.orders[q][nb - 1 - k]
        whole = p.orders[q][nb - k :]

        def make(u):
            slot = lax.rem(u, SLOTS)
            h, c = u // C, lax.rem(u, C)
            to = (me ^ (1 << d), z)
            last = k == nb - 1
            size = p.w if last else wq
            first = c * p.w + (0 if last else q * wq)
            columns = pl.ds(pl.multiple_of(first, wq), size)
            spots = [tuple(every if e in whole else (b if e == d else 0) for e in range(nb)) for b in (0, 1)]
            src, dst = (act.at[(h,) + spot + (every, columns)] for spot in spots)
            if last:
                return remote(src, dst, sems["sl"].at[slot], sems["rl"].at[u], to)
            return remote(src, dst, sems["sa"].at[k, q, slot], sems["ra"].at[k, q, u], to)

        return make

    def issue(make, u):
        @pl.when(u >= SLOTS)
        def _():
            make(u - SLOTS).wait_send()

        make(u).start()

    for i in range(2):
        w_copy(0, i).start()
    for h in range(p.h):
        for pos in range(n):
            x_copy(h, pos).start()
    barrier = pltpu.get_barrier_semaphore()
    for d in range(nb):
        pl.semaphore_signal(barrier, inc=1, device_id=(me ^ (1 << d), z), device_id_type=MESH)
    pl.semaphore_signal(barrier, inc=1, device_id=(me, inward), device_id_type=MESH)

    @pl.when(deep > 0)
    def _():
        pl.semaphore_signal(barrier, inc=1, device_id=(me, outward), device_id_type=MESH)

    pl.semaphore_wait(barrier, nb + 1 + jnp.where(deep > 0, 1, 0))
    for h in range(p.h):
        for pos in range(n):
            x_copy(h, pos).wait()

    def up(c):
        @pl.when(c + 1 < C)
        def _():
            for i in range(2):
                w_copy(c + 1, i).start()

        slot = lax.rem(c, 2)
        columns = pl.ds(pl.multiple_of(c * p.w, p.w), p.w)
        x = xp[...].reshape(p.h * n * rb, p.depth)
        for i, scales in enumerate((gs, us)):
            w_copy(c, i).wait()
            weight = dequant(w[slot, i * p.depth : (i + 1) * p.depth], scales[:, columns])
            part = jnp.dot(x, weight, preferred_element_type=F32).astype(BF16)
            part = part.reshape((p.h,) + (2,) * nb + (rb, p.w))
            for h in range(p.h):
                for q in range(2):
                    ps[(h * C + c,) + (every,) * nb + (q, i)] = part[h, ..., q * wq : (q + 1) * wq]

    def total(u, q, fixed, count):
        value = ps[part_at(u, q, fixed)].astype(F32)
        if count > 0:
            value = value + r0[(u,) + index(fixed, range(1, nb)) + (q,)].astype(F32)
        for k in range(1, count):
            value = value + rk[k - 1][(u, q) + index(fixed, p.left(q, k))].astype(F32)
        return value

    def reduce(s, u):
        if s == 1:
            sum_copy(0, 0)(u).wait_recv()
        for q in range(2):
            if s > 1:
                sum_copy(s - 1, q)(u).wait_recv()
            fixed = {e: 0 for e in p.orders[q][:s]} | {p.orders[q][s]: 1}
            ps[part_at(u, q, fixed)] = total(u, q, fixed, s).astype(BF16)
            issue(sum_copy(s, q), u)

    def activate(u):
        h, c = u // C, lax.rem(u, C)
        for q in range(2):
            sum_copy(nb - 1, q)(u).wait_recv()
            both = total(u, q, {e: 0 for e in range(nb)}, nb)
            gate, up_ = both[0], both[1]
            columns = pl.ds(pl.multiple_of(c * p.w + q * wq, wq), wq)
            act[(h,) + (0,) * nb + (every, columns)] = (gate / (1.0 + jnp.exp(-gate)) * up_).astype(BF16)
            issue(act_copy(0, q), u)

    def gather(k, u):
        for q in range(2):
            act_copy(k - 1, q)(u).wait_recv()
            if k < nb - 1:
                issue(act_copy(k, q), u)
        if k == nb - 1:
            issue(act_copy(k, 0), u)

    def down(v):
        @pl.when(v + 1 < V)
        def _():
            for i in range(2):
                d_copy(v + 1, i).start()

        h = v // J
        slot = lax.rem(v, 2)
        columns = pl.ds(pl.multiple_of(lax.rem(v, J) * wq, wq), wq)
        groups = ds.shape[0] // 2
        value = None
        for i in range(2):
            d_copy(v, i).wait()
            weight = dequant(
                w[slot, : p.k2, i * wq : (i + 1) * wq], ds[i * groups : (i + 1) * groups, columns]
            )
            a = act[(h,) + (every,) * nb + (every, slice(i * p.k2, (i + 1) * p.k2))].reshape(n * rb, p.k2)
            term = jnp.dot(a, weight, preferred_element_type=F32)
            value = term if value is None else value + term
        zs[v] = value.astype(BF16)

        @pl.when(deep == 0)
        def _():
            z_in(v).start()

    def z_in(v):
        return remote(zs.at[v], zr.at[v], sems["zs"].at[v], sems["zr"].at[v], (me, inward))

    def z_cross(v):
        return remote(zs.at[v], zx.at[v], sems["zs"].at[v], sems["zx"].at[v], (me, inward))

    def z_out(v):
        return remote(zf.at[v], zf.at[v], sems["zo"].at[v], sems["zf"].at[v], (me, outward))

    def put(v):
        h = v // J
        columns = pl.ds(pl.multiple_of(lax.rem(v, J) * wq, wq), wq)
        for pos in range(n):
            out[me ^ p.mask(pos), h, :, columns] = zf[v, pos * rb : (pos + 1) * rb]

    def z_step(k, v):
        if k < p.mid:

            @pl.when(deep == k)
            def _():
                z_in(v).wait_recv()
                zs[v] = (zs[v].astype(F32) + zr[v].astype(F32)).astype(BF16)
                if k < p.mid - 1:
                    z_in(v).start()
                else:
                    z_cross(v).start()
        elif k == p.mid:

            @pl.when(deep == p.mid - 1)
            def _():
                z_cross(v).wait_recv()
                h = v // J
                columns = pl.ds(pl.multiple_of(lax.rem(v, J) * wq, wq), wq)
                own = xp[h, :, :, columns].reshape(n * rb, wq).astype(F32)
                zf[v] = (zs[v].astype(F32) + zx[v].astype(F32) + own).astype(BF16)
                if p.mid > 1:
                    z_out(v).start()
                put(v)
        else:
            at = 2 * p.mid - 1 - k

            @pl.when(deep == at)
            def _():
                z_out(v).wait_recv()
                if at > 0:
                    z_out(v).start()
                put(v)

    first_down = C + 2 * nb

    def item(t, run):
        h, j = jnp.maximum(t, 0) // C, lax.rem(jnp.maximum(t, 0), C)

        @pl.when((t >= 0) & (h < p.h) & (j < J))
        def _():
            run(h * J + j)

    def unit(u, run):
        @pl.when((u >= 0) & (u < U))
        def _():
            run(u)

    def step(t, carry):
        @pl.when(t < C)
        def _():
            up(t)

        @pl.when(t == C)
        def _():
            for i in range(2):
                d_copy(0, i).start()

        item(t - first_down, down)
        unit(t, lambda u: issue(sum_copy(0, 0), u))
        for s in range(1, nb):
            unit(t - s, functools.partial(reduce, s))
        unit(t - nb, activate)
        for k in range(1, nb):
            unit(t - nb - k, functools.partial(gather, k))
        unit(t - 2 * nb, lambda u: act_copy(nb - 1, 0)(u).wait_recv())
        for k in range(1, 2 * p.mid):
            item(t - first_down - k, functools.partial(z_step, k))
        return carry

    lax.fori_loop(0, first_down + (p.h - 1) * C + J + 2 * p.mid - 1, step, 0)

    for u in range(U - SLOTS, U):
        sum_copy(0, 0)(u).wait_send()
        act_copy(nb - 1, 0)(u).wait_send()
        for q in range(2):
            for s in range(1, nb):
                sum_copy(s, q)(u).wait_send()
            for k in range(nb - 1):
                act_copy(k, q)(u).wait_send()

    def finish(v, carry):
        z_in(v).wait_send()

        @pl.when(deep > 0)
        def _():
            z_out(v).wait_send()

        return carry

    lax.fori_loop(0, V, finish, 0)


def body(n, nz, states, gc, gs, uc, us, dc, ds):
    rows, depth = states.shape
    hidden = gc.shape[1]
    p = Plan(n, nz, rows, depth, hidden)
    nb, U, V, rb, wq = p.nb, p.u, p.v, p.rb, p.wq
    dma = pltpu.SemaphoreType.DMA
    vmem = pl.BlockSpec(memory_space=pltpu.VMEM)
    hbm = pl.BlockSpec(memory_space=pl.ANY)
    two = (2,) * nb
    item = (V, n * rb, wq)
    scratch = [
        pltpu.VMEM((p.h, n, rb, depth), BF16),
        pltpu.VMEM((2, p.wrows, p.w), BF16),
        pltpu.VMEM((U,) + two + (2, 2, rb, wq), BF16),
        pltpu.VMEM((U,) + two[1:] + (2, 2, rb, wq), BF16),
        [pltpu.VMEM((U, 2) + two[k + 1 :] + (2, rb, wq), BF16) for k in range(1, nb)],
        pltpu.VMEM((p.h,) + two + (rb, hidden), BF16),
        pltpu.VMEM(item, BF16),
        pltpu.VMEM(item, BF16),
        pltpu.VMEM(item, BF16),
        pltpu.VMEM(item, BF16),
        {
            "x": dma((p.h * n,)),
            "w": dma((2, 2)),
            "s0": dma((SLOTS,)),
            "r0": dma((U,)),
            "sk": dma((nb - 1, 2, SLOTS)),
            "rk": dma((nb - 1, 2, U)),
            "sa": dma((nb - 1, 2, SLOTS)),
            "ra": dma((nb - 1, 2, U)),
            "sl": dma((SLOTS,)),
            "rl": dma((U,)),
            "zs": dma((V,)),
            "zr": dma((V,)),
            "zx": dma((V,)),
            "zo": dma((V,)),
            "zf": dma((V,)),
        },
    ]
    out = pl.pallas_call(
        functools.partial(kernel, p),
        out_shape=jax.ShapeDtypeStruct((n, p.h, rb, depth), BF16),
        in_specs=[hbm] * 4 + [vmem] * 3,
        out_specs=vmem,
        scratch_shapes=scratch,
        compiler_params=pltpu.CompilerParams(collective_id=0, has_side_effects=True, vmem_limit_bytes=67043328),
        cost_estimate=pl.CostEstimate(
            flops=6 * rows * depth * hidden, bytes_accessed=8 * depth * hidden, transcendentals=0
        ),
        name="mlp",
    )(states.reshape(n, p.h, rb, depth), gc, uc, dc, gs, us, ds)
    return out.reshape(rows, depth)


def solution(mesh):
    in_specs = (
        P(None, "mp"),
        P("mp", "hidden"),
        P("mp", "hidden"),
        P("mp", "hidden"),
        P("mp", "hidden"),
        P("hidden", "mp"),
        P("hidden", "mp"),
    )
    return jax.shard_map(
        functools.partial(body, mesh.shape["mp"], mesh.shape["hidden"]),
        mesh=mesh,
        in_specs=in_specs,
        out_specs=P(None, "mp"),
        check_vma=False,
    )
```

```python
import functools

import jax
import jax.numpy as jnp
from jax import lax
from jax.experimental import pallas as pl
from jax.experimental.pallas import tpu as pltpu
from jax.sharding import PartitionSpec as P

F32, BF16 = jnp.float32, jnp.bfloat16
MESH = pl.DeviceIdType.MESH
SLOTS = 4
SPLITS = ((2, 1, 1), (1, 1))
PACES = (1, 2, 2)
EARLY = (0, 0, 0)
FIRST = 0
LAGS = (4, 6, 6)


def dequant(codes, scales):
    depth, columns = codes.shape
    groups = scales.shape[0]
    blocks = codes.astype(F32).reshape(groups, depth // groups, columns)
    return (blocks * scales.reshape(groups, 1, columns)).reshape(depth, columns).astype(BF16)


class Split:
    def __init__(self, rb, row, off, runs, lag, pace):
        self.rb, self.row, self.off, self.runs, self.lag = rb, row, off, runs, lag
        self.send, self.recv = 2 * pace, 4 * pace


class Plan:
    def __init__(self, n, nz, rows, depth, hidden):
        self.n, self.nz, self.depth, self.hidden = n, nz, depth, hidden
        self.nb = n.bit_length() - 1
        self.rows = rows
        self.w = next(t for t in (512, 256) if hidden % t == 0)
        self.wq = self.w // 2
        self.c = hidden // self.w
        self.j = depth // self.wq
        self.k2 = hidden // 2
        self.wrows = max(2 * depth, self.k2)
        dims = list(range(self.nb))
        self.orders = (dims, dims[:1] + dims[:0:-1])
        self.mid = nz // 2
        rb = rows // n
        parts = next((p for p in SPLITS if all(rb * a % (16 * sum(p)) == 0 for a in p)), (1,))
        self.splits = []
        row, free, tick = 0, 0, 0
        for i, a in enumerate(parts):
            size = rb * a // sum(parts)
            pace = PACES[i] if i else 1
            early = min(EARLY[i], self.c) if i else 0
            runs = []
            if early:
                runs.append((0, early, FIRST, 1))
            if early < self.c:
                runs.append((early, self.c, tick, pace))
                tick += -(-(self.c - early) // pace)
            split = Split(size, row, n * row, runs, LAGS[i], pace)
            split.down = max(tick + 2 * self.nb, free)
            free = split.down + self.j
            self.splits.append(split)
            row += size
        self.cuts = {0, self.c} | {s.down for s in self.splits} | {s.down + self.j for s in self.splits}
        self.ticks = max(s.down + self.j - 1 + self.after(s, 2 * self.mid - 1) for s in self.splits) + 1

    def after(self, s, k):
        return -(-s.lag * k // 2)

    def left(self, q, k):
        return sorted(set(range(self.nb)) - set(self.orders[q][: k + 1]))

    def mask(self, pos):
        return sum(((pos >> (self.nb - 1 - d)) & 1) << d for d in range(self.nb))


def kernel(p, x_hbm, gc, uc, dc, gs, us, ds, out_hbm, out, xp, w, per, sems):
    n, nb, C, J, wq = p.n, p.nb, p.c, p.j, p.wq
    me = lax.axis_index("mp").astype(jnp.int32)
    z = lax.axis_index("hidden").astype(jnp.int32)
    nz = p.nz
    on_left = z < p.mid
    deep = jnp.where(on_left, z, nz - 1 - z)
    inward = jnp.where(on_left, z + 1, z - 1)
    outward = jnp.where(on_left, z - 1, z + 1)
    every = slice(None)

    def index(fixed, dims):
        return tuple(fixed.get(d, every) for d in dims)

    def columns_of(c):
        return pl.ds(pl.multiple_of(c * p.w, p.w), p.w)

    def columns_at(j):
        return pl.ds(pl.multiple_of(j * wq, wq), wq)

    def x_copy(i, pos):
        s = p.splits[i]
        return pltpu.make_async_copy(
            x_hbm.at[me ^ p.mask(pos), pl.ds(s.row, s.rb)],
            xp.at[pl.ds(s.off + pos * s.rb, s.rb)],
            sems["x"].at[i * n + pos],
        )

    def w_copy(c, i):
        slot = lax.rem(c, 2)
        return pltpu.make_async_copy(
            (gc, uc)[i].at[:, columns_of(c)], w.at[slot, pl.ds(i * p.depth, p.depth)], sems["w"].at[slot, i]
        )

    def d_copy(v, i):
        slot = lax.rem(v, 2)
        return pltpu.make_async_copy(
            dc.at[pl.ds(i * p.k2, p.k2), columns_at(lax.rem(v, J))],
            w.at[slot, pl.ds(0, p.k2), pl.ds(i * wq, wq)],
            sems["w"].at[slot, i],
        )

    def out_copy(i, j):
        s = p.splits[i]
        part = (every, pl.ds(s.row, s.rb), columns_at(j))
        return pltpu.make_async_copy(out.at[part], out_hbm.at[part], per[i]["sem"]["o"].at[lax.rem(j, SLOTS)])

    def remote(src, dst, send, recv, to):
        return pltpu.make_async_remote_copy(
            src_ref=src, dst_ref=dst, send_sem=send, recv_sem=recv, device_id=to, device_id_type=MESH
        )

    def part_at(c, q, fixed):
        return (c,) + index(fixed, range(nb)) + (q,)

    def sum_copy(i, s, q):
        d = p.orders[q][s]
        ps, r0, rk, sem = per[i]["ps"], per[i]["r0"], per[i]["rk"], per[i]["sem"]

        def make(c):
            slot, got = lax.rem(c, p.splits[i].send), lax.rem(c, p.splits[i].recv)
            to = (me ^ (1 << d), z)
            if s == 0:
                return remote(ps.at[c, 1], r0.at[c], sem["s0"].at[slot], sem["r0"].at[got], to)
            fixed = {e: 0 for e in p.orders[q][:s]} | {d: 1}
            return remote(
                ps.at[part_at(c, q, fixed)],
                rk[s - 1].at[c, q],
                sem["sk"].at[s - 1, q, slot],
                sem["rk"].at[s - 1, q, got],
                to,
            )

        return make

    def act_copy(i, k, q):
        d = p.orders[q][nb - 1 - k]
        whole = p.orders[q][nb - k :]
        act, sem = per[i]["act"], per[i]["sem"]

        def make(c):
            slot, got = lax.rem(c, p.splits[i].send), lax.rem(c, p.splits[i].recv)
            to = (me ^ (1 << d), z)
            last = k == nb - 1
            size = p.w if last else wq
            first = c * p.w + (0 if last else q * wq)
            columns = pl.ds(pl.multiple_of(first, wq), size)
            spots = [tuple(every if e in whole else (b if e == d else 0) for e in range(nb)) for b in (0, 1)]
            src, dst = (act.at[spot + (every, columns)] for spot in spots)
            if last:
                return remote(src, dst, sem["sl"].at[slot], sem["rl"].at[got], to)
            return remote(src, dst, sem["sa"].at[k, q, slot], sem["ra"].at[k, q, got], to)

        return make

    def issue(make, c, slots):
        @pl.when(c >= slots)
        def _():
            make(c - slots).wait_send()

        make(c).start()

    for i in range(len(p.splits)):
        for pos in range(n):
            x_copy(i, pos).start()
    for i in range(2):
        w_copy(0, i).start()
    barrier = pltpu.get_barrier_semaphore()
    for d in range(nb):
        pl.semaphore_signal(barrier, inc=1, device_id=(me ^ (1 << d), z), device_id_type=MESH)
    pl.semaphore_signal(barrier, inc=1, device_id=(me, inward), device_id_type=MESH)

    @pl.when(deep > 0)
    def _():
        pl.semaphore_signal(barrier, inc=1, device_id=(me, outward), device_id_type=MESH)

    for i in range(len(p.splits)):
        for pos in range(n):
            x_copy(i, pos).wait()
    pl.semaphore_wait(barrier, nb + 1 + jnp.where(deep > 0, 1, 0))

    def up(c):
        @pl.when(c + 1 < C)
        def _():
            for i in range(2):
                w_copy(c + 1, i).start()

        slot = lax.rem(c, 2)
        for i, scales in enumerate((gs, us)):
            w_copy(c, i).wait()
            weight = dequant(w[slot, i * p.depth : (i + 1) * p.depth], scales[:, columns_of(c)])
            part = jnp.dot(xp[...], weight, preferred_element_type=F32).astype(BF16)
            for s, own in zip(p.splits, per):
                rows = part[s.off : s.off + n * s.rb].reshape((2,) * nb + (s.rb, p.w))
                for q in range(2):
                    own["ps"][(c,) + (every,) * nb + (q, i)] = rows[..., q * wq : (q + 1) * wq]

    def total(own, c, q, fixed, count):
        value = own["ps"][part_at(c, q, fixed)].astype(F32)
        if count > 0:
            value = value + own["r0"][(c,) + index(fixed, range(1, nb)) + (q,)].astype(F32)
        for k in range(1, count):
            value = value + own["rk"][k - 1][(c, q) + index(fixed, p.left(q, k))].astype(F32)
        return value

    def reduce(i, s, c):
        if s == 1:
            sum_copy(i, 0, 0)(c).wait_recv()
        for q in range(2):
            if s > 1:
                sum_copy(i, s - 1, q)(c).wait_recv()
            fixed = {e: 0 for e in p.orders[q][:s]} | {p.orders[q][s]: 1}
            per[i]["ps"][part_at(c, q, fixed)] = total(per[i], c, q, fixed, s).astype(BF16)
            issue(sum_copy(i, s, q), c, p.splits[i].send)

    def activate(i, c):
        for q in range(2):
            sum_copy(i, nb - 1, q)(c).wait_recv()
            both = total(per[i], c, q, {e: 0 for e in range(nb)}, nb)
            gate, up_ = both[0], both[1]
            columns = pl.ds(pl.multiple_of(c * p.w + q * wq, wq), wq)
            per[i]["act"][(0,) * nb + (every, columns)] = (gate / (1.0 + jnp.exp(-gate)) * up_).astype(BF16)
            issue(act_copy(i, 0, q), c, p.splits[i].send)

    def gather(i, k, c):
        for q in range(2):
            act_copy(i, k - 1, q)(c).wait_recv()
            if k < nb - 1:
                issue(act_copy(i, k, q), c, p.splits[i].send)
        if k == nb - 1:
            issue(act_copy(i, k, 0), c, p.splits[i].send)

    def down(i, j):
        v = i * J + j

        @pl.when(v + 1 < J * len(p.splits))
        def _():
            for k in range(2):
                d_copy(v + 1, k).start()

        own = per[i]
        slot = lax.rem(v, 2)
        groups = ds.shape[0] // 2
        value = None
        for k in range(2):
            d_copy(v, k).wait()
            weight = dequant(
                w[slot, : p.k2, k * wq : (k + 1) * wq], ds[k * groups : (k + 1) * groups, columns_at(j)]
            )
            a = own["act"][(every,) * nb + (every, slice(k * p.k2, (k + 1) * p.k2))]
            term = jnp.dot(a.reshape(n * p.splits[i].rb, p.k2), weight, preferred_element_type=F32)
            value = term if value is None else value + term
        own["zs"][j] = value.astype(BF16)

        @pl.when(deep == 0)
        def _():
            issue(functools.partial(z_in, i), j, SLOTS)

    def z_in(i, j):
        own, sem = per[i], per[i]["sem"]
        return remote(own["zs"].at[j], own["zr"].at[j], sem["zs"].at[lax.rem(j, SLOTS)], sem["zr"].at[j], (me, inward))

    def z_cross(i, j):
        own, sem = per[i], per[i]["sem"]
        return remote(own["zs"].at[j], own["zx"].at[j], sem["zs"].at[lax.rem(j, SLOTS)], sem["zx"].at[j], (me, inward))

    def z_out(i, j):
        own, sem = per[i], per[i]["sem"]
        return remote(own["zf"].at[j], own["zf"].at[j], sem["zo"].at[lax.rem(j, SLOTS)], sem["zf" if p.mid > 2 else "zr"].at[j], (me, outward))

    def put(i, j):
        s = p.splits[i]
        for pos in range(n):
            out[me ^ p.mask(pos), s.row : s.row + s.rb, columns_at(j)] = per[i]["zf"][j, pos * s.rb : (pos + 1) * s.rb]

        @pl.when(j >= SLOTS)
        def _():
            out_copy(i, j - SLOTS).wait()

        out_copy(i, j).start()

    def z_step(i, k, j):
        zs, zr, zx, zf = (per[i][key] for key in ("zs", "zr", "zx", "zf"))
        if k < p.mid:

            @pl.when(deep == k)
            def _():
                z_in(i, j).wait_recv()
                zs[j] = (zs[j].astype(F32) + zr[j].astype(F32)).astype(BF16)
                if k < p.mid - 1:
                    issue(functools.partial(z_in, i), j, SLOTS)
                else:
                    issue(functools.partial(z_cross, i), j, SLOTS)
        elif k == p.mid:

            @pl.when(deep == p.mid - 1)
            def _():
                z_cross(i, j).wait_recv()
                s = p.splits[i]
                own = xp[s.off : s.off + n * s.rb, columns_at(j)].astype(F32)
                zf[j] = (zs[j].astype(F32) + zx[j].astype(F32) + own).astype(BF16)
                if p.mid > 1:
                    issue(functools.partial(z_out, i), j, SLOTS)
                put(i, j)
        else:
            at = 2 * p.mid - 1 - k

            @pl.when(deep == at)
            def _():
                z_out(i, j).wait_recv()
                if at > 0:
                    issue(functools.partial(z_out, i), j, SLOTS)
                put(i, j)

    def shift(s, k):
        return [(first, last, start + k, pace) for first, last, start, pace in s.runs]

    def each(t, begin, end, runs, run):
        for first, last, start, pace in runs:
            for g in range(pace):
                stop = start - (g - (last - first)) // pace
                if begin >= stop or end <= start:
                    continue
                i = first + (t - start) * pace + g
                if start <= begin and end <= stop:
                    run(i)
                else:
                    pl.when((t >= start) & (t < stop))(functools.partial(run, i))

    def step(begin, end, t, carry):
        act_ = functools.partial(each, t, begin, end)
        if end <= C:
            up(t)
        for i, s in enumerate(p.splits):
            act_([(0, J, s.down, 1)], functools.partial(down, i))
            act_(shift(s, 0), lambda c, i=i: issue(sum_copy(i, 0, 0), c, p.splits[i].send))
        for k in range(1, 2 * nb + 1):
            for i, s in enumerate(p.splits):
                if k < nb:
                    run = functools.partial(reduce, i, k)
                elif k == nb:
                    run = functools.partial(activate, i)
                elif k < 2 * nb:
                    run = functools.partial(gather, i, k - nb)
                else:
                    run = lambda c, i=i: act_copy(i, nb - 1, 0)(c).wait_recv()
                act_(shift(s, k), run)
        for k in range(1, 2 * p.mid):
            for i, s in enumerate(p.splits):
                act_([(0, J, s.down + p.after(s, k), 1)], functools.partial(z_step, i, k))
        return carry

    cuts = sorted(c for c in p.cuts if c < p.ticks) + [p.ticks]
    for begin, end in zip(cuts, cuts[1:]):
        if begin == C:
            for i in range(2):
                d_copy(0, i).start()
        lax.fori_loop(begin, end, functools.partial(step, begin, end), 0)

    for i in range(len(p.splits)):
        for c in range(max(C - p.splits[i].send, 0), C):
            sum_copy(i, 0, 0)(c).wait_send()
            act_copy(i, nb - 1, 0)(c).wait_send()
            for q in range(2):
                for s in range(1, nb):
                    sum_copy(i, s, q)(c).wait_send()
                for k in range(nb - 1):
                    act_copy(i, k, q)(c).wait_send()

        def finish(j, carry, i=i):
            z_in(i, j).wait_send()
            out_copy(i, j).wait()

            @pl.when(deep > 0)
            def _():
                z_out(i, j).wait_send()

            return carry

        lax.fori_loop(max(J - SLOTS, 0), J, finish, 0)


def body(n, nz, states, gc, gs, uc, us, dc, ds):
    rows, depth = states.shape
    hidden = gc.shape[1]
    p = Plan(n, nz, rows, depth, hidden)
    nb, C, J, wq = p.nb, p.c, p.j, p.wq
    dma = pltpu.SemaphoreType.DMA
    vmem = pl.BlockSpec(memory_space=pltpu.VMEM)
    hbm = pl.BlockSpec(memory_space=pl.ANY)
    two = (2,) * nb

    def own(s):
        item = pltpu.VMEM((J, n * s.rb, wq), BF16)
        return {
            "ps": pltpu.VMEM((C,) + two + (2, 2, s.rb, wq), BF16),
            "r0": pltpu.VMEM((C,) + two[1:] + (2, 2, s.rb, wq), BF16),
            "rk": [pltpu.VMEM((C, 2) + two[k + 1 :] + (2, s.rb, wq), BF16) for k in range(1, nb)],
            "act": pltpu.VMEM(two + (s.rb, hidden), BF16),
            "zs": item,
            "zr": item,
            "zx": item,
            "zf": item,
            "sem": {
                "s0": dma((s.send,)),
                "r0": dma((s.recv,)),
                "sk": dma((nb - 1, 2, s.send)),
                "rk": dma((nb - 1, 2, s.recv)),
                "sa": dma((nb - 1, 2, s.send)),
                "ra": dma((nb - 1, 2, s.recv)),
                "sl": dma((s.send,)),
                "rl": dma((s.recv,)),
                "zs": dma((SLOTS,)),
                "zr": dma((J,)),
                "zx": dma((J,)),
                "zo": dma((SLOTS,)),
                "zf": dma((J if p.mid > 2 else 1,)),
                "o": dma((SLOTS,)),
            },
        }

    out = pl.pallas_call(
        functools.partial(kernel, p),
        out_shape=jax.ShapeDtypeStruct((n, rows // n, depth), BF16),
        in_specs=[hbm] * 4 + [vmem] * 3,
        out_specs=hbm,
        scratch_shapes=[
            pltpu.VMEM((n, rows // n, depth), BF16),
            pltpu.VMEM((rows, depth), BF16),
            pltpu.VMEM((2, p.wrows, p.w), BF16),
            [own(s) for s in p.splits],
            {"x": dma((len(p.splits) * n,)), "w": dma((2, 2))},
        ],
        compiler_params=pltpu.CompilerParams(collective_id=0, has_side_effects=True, vmem_limit_bytes=67043328),
        cost_estimate=pl.CostEstimate(
            flops=6 * rows * depth * hidden, bytes_accessed=8 * depth * hidden, transcendentals=0
        ),
        name="mlp",
    )(states.reshape(n, rows // n, depth), gc, uc, dc, gs, us, ds)
    return out.reshape(rows, depth)


def solution(mesh):
    in_specs = (
        P(None, "mp"),
        P("mp", "hidden"),
        P("mp", "hidden"),
        P("mp", "hidden"),
        P("mp", "hidden"),
        P("hidden", "mp"),
        P("hidden", "mp"),
    )
    return jax.shard_map(
        functools.partial(body, mesh.shape["mp"], mesh.shape["hidden"]),
        mesh=mesh,
        in_specs=in_specs,
        out_specs=P(None, "mp"),
        check_vma=False,
    )
```

```python
import functools

import jax
import jax.numpy as jnp
from jax import lax
from jax.experimental import pallas as pl
from jax.experimental.pallas import tpu as pltpu
from jax.sharding import PartitionSpec as P

F32, BF16 = jnp.float32, jnp.bfloat16
MESH = pl.DeviceIdType.MESH
SLOTS = 4
SPLITS = ((2, 1, 1), (1, 1))
PACES = (1, 2, 2)
SLOW = (0, 3, 0)
LAGS = (4, 6, 7)


def dequant(codes, scales):
    depth, columns = codes.shape
    groups = scales.shape[0]
    blocks = codes.astype(F32).reshape(groups, depth // groups, columns)
    return (blocks * scales.reshape(groups, 1, columns)).reshape(depth, columns).astype(BF16)


class Split:
    def __init__(self, rb, row, off, runs, lag, pace):
        self.rb, self.row, self.off, self.runs, self.lag = rb, row, off, runs, lag
        self.send, self.recv = 2 * pace, 4 * pace


class Plan:
    def __init__(self, n, nz, rows, depth, hidden):
        self.n, self.nz, self.depth, self.hidden = n, nz, depth, hidden
        self.nb = n.bit_length() - 1
        self.rows = rows
        self.w = next(t for t in (512, 256) if hidden % t == 0)
        self.wq = self.w // 2
        self.c = hidden // self.w
        self.j = depth // self.wq
        self.k2 = hidden // 2
        self.wrows = max(2 * depth, self.k2)
        dims = list(range(self.nb))
        self.orders = (dims, dims[:1] + dims[:0:-1])
        self.mid = nz // 2
        rb = rows // n
        parts = next((p for p in SPLITS if all(rb * a % (16 * sum(p)) == 0 for a in p)), (1,))
        self.splits = []
        row, free, tick = 0, 0, 0
        for i, a in enumerate(parts):
            size = rb * a // sum(parts)
            pace = PACES[i] if i else 1
            slow = min(SLOW[i], self.c) if i else 0
            runs = []
            if slow:
                runs.append((0, slow, tick, 1))
                tick += slow
            if slow < self.c:
                runs.append((slow, self.c, tick, pace))
                tick += -(-(self.c - slow) // pace)
            split = Split(size, row, n * row, runs, LAGS[i], pace)
            split.down = max(tick + 2 * self.nb, free)
            free = split.down + self.j
            self.splits.append(split)
            row += size
        self.cuts = {0, 1, self.c} | {s.down for s in self.splits} | {s.down + self.j for s in self.splits}
        self.ticks = max(s.down + self.j - 1 + self.after(s, 2 * self.mid - 1) for s in self.splits) + 1

    def after(self, s, k):
        return -(-s.lag * k // 2)

    def left(self, q, k):
        return sorted(set(range(self.nb)) - set(self.orders[q][: k + 1]))

    def mask(self, pos):
        return sum(((pos >> (self.nb - 1 - d)) & 1) << d for d in range(self.nb))


def kernel(p, x_hbm, gc, uc, dc, gs, us, ds, out_hbm, out, xp, w, per, sems):
    n, nb, C, J, wq = p.n, p.nb, p.c, p.j, p.wq
    me = lax.axis_index("mp").astype(jnp.int32)
    z = lax.axis_index("hidden").astype(jnp.int32)
    nz = p.nz
    on_left = z < p.mid
    deep = jnp.where(on_left, z, nz - 1 - z)
    inward = jnp.where(on_left, z + 1, z - 1)
    outward = jnp.where(on_left, z - 1, z + 1)
    every = slice(None)

    def index(fixed, dims):
        return tuple(fixed.get(d, every) for d in dims)

    def columns_of(c):
        return pl.ds(pl.multiple_of(c * p.w, p.w), p.w)

    def columns_at(j):
        return pl.ds(pl.multiple_of(j * wq, wq), wq)

    def x_copy(i, pos):
        s = p.splits[i]
        return pltpu.make_async_copy(
            x_hbm.at[me ^ p.mask(pos), pl.ds(s.row, s.rb)],
            xp.at[pl.ds(s.off + pos * s.rb, s.rb)],
            sems["x"].at[i * n + pos],
        )

    def w_copy(c, i):
        slot = lax.rem(c, 2)
        return pltpu.make_async_copy(
            (gc, uc)[i].at[:, columns_of(c)], w.at[slot, pl.ds(i * p.depth, p.depth)], sems["w"].at[slot, i]
        )

    def d_copy(v, i):
        slot = lax.rem(v, 2)
        return pltpu.make_async_copy(
            dc.at[pl.ds(i * p.k2, p.k2), columns_at(lax.rem(v, J))],
            w.at[slot, pl.ds(0, p.k2), pl.ds(i * wq, wq)],
            sems["w"].at[slot, i],
        )

    def out_copy(i, j):
        s = p.splits[i]
        part = (every, pl.ds(s.row, s.rb), columns_at(j))
        return pltpu.make_async_copy(out.at[part], out_hbm.at[part], per[i]["sem"]["o"].at[lax.rem(j, SLOTS)])

    def remote(src, dst, send, recv, to):
        return pltpu.make_async_remote_copy(
            src_ref=src, dst_ref=dst, send_sem=send, recv_sem=recv, device_id=to, device_id_type=MESH
        )

    def part_at(c, q, fixed):
        return (c,) + index(fixed, range(nb)) + (q,)

    def sum_copy(i, s, q):
        d = p.orders[q][s]
        ps, r0, rk, sem = per[i]["ps"], per[i]["r0"], per[i]["rk"], per[i]["sem"]

        def make(c):
            slot, got = lax.rem(c, p.splits[i].send), lax.rem(c, p.splits[i].recv)
            to = (me ^ (1 << d), z)
            if s == 0:
                return remote(ps.at[c, 1], r0.at[c], sem["s0"].at[slot], sem["r0"].at[got], to)
            fixed = {e: 0 for e in p.orders[q][:s]} | {d: 1}
            return remote(
                ps.at[part_at(c, q, fixed)],
                rk[s - 1].at[c, q],
                sem["sk"].at[s - 1, slot],
                sem["rk"].at[s - 1, got],
                to,
            )

        return make

    def act_copy(i, k, q):
        d = p.orders[q][nb - 1 - k]
        whole = p.orders[q][nb - k :]
        act, sem = per[i]["act"], per[i]["sem"]

        def make(c):
            slot, got = lax.rem(c, p.splits[i].send), lax.rem(c, p.splits[i].recv)
            to = (me ^ (1 << d), z)
            last = k == nb - 1
            size = p.w if last else wq
            first = c * p.w + (0 if last else q * wq)
            columns = pl.ds(pl.multiple_of(first, wq), size)
            spots = [tuple(every if e in whole else (b if e == d else 0) for e in range(nb)) for b in (0, 1)]
            src, dst = (act.at[spot + (every, columns)] for spot in spots)
            if last:
                return remote(src, dst, sem["sl"].at[slot], sem["rl"].at[got], to)
            return remote(src, dst, sem["sa"].at[k, slot], sem["ra"].at[k, got], to)

        return make

    def issue(make, c, slots):
        @pl.when(c >= slots)
        def _():
            make(c - slots).wait_send()

        make(c).start()

    def sums_wait(i, s, c, key, slots):
        both = per[i]["rk"][s - 1].at[c]
        pltpu.make_async_copy(both, both, per[i]["sem"][key].at[s - 1, lax.rem(c, slots)]).wait()

    def acts_wait(i, k, c, key, slots):
        both = per[i]["act"].at[(0,) * (nb - k) + (every,) * k + (every, columns_of(c))]
        pltpu.make_async_copy(both, both, per[i]["sem"][key].at[k, lax.rem(c, slots)]).wait()

    def make_room(wait, i, k, c, key):
        slots = p.splits[i].send

        @pl.when(c >= slots)
        def _():
            wait(i, k, c - slots, key, slots)

    for i in range(len(p.splits)):
        for pos in range(n):
            x_copy(i, pos).start()
    for i in range(2):
        w_copy(0, i).start()
    barrier = pltpu.get_barrier_semaphore()
    for d in range(nb):
        pl.semaphore_signal(barrier, inc=1, device_id=(me ^ (1 << d), z), device_id_type=MESH)
    pl.semaphore_signal(barrier, inc=1, device_id=(me, inward), device_id_type=MESH)

    @pl.when(deep > 0)
    def _():
        pl.semaphore_signal(barrier, inc=1, device_id=(me, outward), device_id_type=MESH)

    for i in range(len(p.splits)):
        for pos in range(n):
            x_copy(i, pos).wait()

    def up(c):
        @pl.when(c + 1 < C)
        def _():
            for i in range(2):
                w_copy(c + 1, i).start()

        slot = lax.rem(c, 2)
        for i, scales in enumerate((gs, us)):
            w_copy(c, i).wait()
            weight = dequant(w[slot, i * p.depth : (i + 1) * p.depth], scales[:, columns_of(c)])
            part = jnp.dot(xp[...], weight, preferred_element_type=F32).astype(BF16)
            for s, own in zip(p.splits, per):
                rows = part[s.off : s.off + n * s.rb].reshape((2,) * nb + (s.rb, p.w))
                for q in range(2):
                    own["ps"][(c,) + (every,) * nb + (q, i)] = rows[..., q * wq : (q + 1) * wq]

    def total(own, c, q, fixed, count):
        value = own["ps"][part_at(c, q, fixed)].astype(F32)
        if count > 0:
            value = value + own["r0"][(c,) + index(fixed, range(1, nb)) + (q,)].astype(F32)
        for k in range(1, count):
            value = value + own["rk"][k - 1][(c, q) + index(fixed, p.left(q, k))].astype(F32)
        return value

    def reduce(i, s, c):
        if s == 1:
            sum_copy(i, 0, 0)(c).wait_recv()
        else:
            sums_wait(i, s - 1, c, "rk", p.splits[i].recv)
        make_room(sums_wait, i, s, c, "sk")
        for q in range(2):
            fixed = {e: 0 for e in p.orders[q][:s]} | {p.orders[q][s]: 1}
            per[i]["ps"][part_at(c, q, fixed)] = total(per[i], c, q, fixed, s).astype(BF16)
            sum_copy(i, s, q)(c).start()

    def activate(i, c):
        sums_wait(i, nb - 1, c, "rk", p.splits[i].recv)
        make_room(acts_wait, i, 0, c, "sa")
        for q in range(2):
            both = total(per[i], c, q, {e: 0 for e in range(nb)}, nb)
            gate, up_ = both[0], both[1]
            columns = pl.ds(pl.multiple_of(c * p.w + q * wq, wq), wq)
            per[i]["act"][(0,) * nb + (every, columns)] = (gate / (1.0 + jnp.exp(-gate)) * up_).astype(BF16)
            act_copy(i, 0, q)(c).start()

    def gather(i, k, c):
        acts_wait(i, k - 1, c, "ra", p.splits[i].recv)
        if k < nb - 1:
            make_room(acts_wait, i, k, c, "sa")
            for q in range(2):
                act_copy(i, k, q)(c).start()
        else:
            issue(act_copy(i, k, 0), c, p.splits[i].send)

    def down(i, j):
        v = i * J + j

        @pl.when(v + 1 < J * len(p.splits))
        def _():
            for k in range(2):
                d_copy(v + 1, k).start()

        own = per[i]
        slot = lax.rem(v, 2)
        groups = ds.shape[0] // 2
        value = None
        for k in range(2):
            d_copy(v, k).wait()
            weight = dequant(
                w[slot, : p.k2, k * wq : (k + 1) * wq], ds[k * groups : (k + 1) * groups, columns_at(j)]
            )
            a = own["act"][(every,) * nb + (every, slice(k * p.k2, (k + 1) * p.k2))]
            term = jnp.dot(a.reshape(n * p.splits[i].rb, p.k2), weight, preferred_element_type=F32)
            value = term if value is None else value + term
        own["zs"][j] = value.astype(BF16)

        @pl.when(deep == 0)
        def _():
            issue(functools.partial(z_in, i), j, SLOTS)

    def z_in(i, j):
        own, sem = per[i], per[i]["sem"]
        return remote(own["zs"].at[j], own["zr"].at[j], sem["zs"].at[lax.rem(j, SLOTS)], sem["zr"].at[j], (me, inward))

    def z_cross(i, j):
        own, sem = per[i], per[i]["sem"]
        return remote(own["zs"].at[j], own["zx"].at[j], sem["zs"].at[lax.rem(j, SLOTS)], sem["zx"].at[j], (me, inward))

    def z_out(i, j):
        own, sem = per[i], per[i]["sem"]
        return remote(own["zf"].at[j], own["zf"].at[j], sem["zo"].at[lax.rem(j, SLOTS)], sem["zf" if p.mid > 2 else "zr"].at[j], (me, outward))

    def put(i, j):
        s = p.splits[i]
        for pos in range(n):
            out[me ^ p.mask(pos), s.row : s.row + s.rb, columns_at(j)] = per[i]["zf"][j, pos * s.rb : (pos + 1) * s.rb]

        @pl.when(j >= SLOTS)
        def _():
            out_copy(i, j - SLOTS).wait()

        out_copy(i, j).start()

    def z_step(i, k, j):
        zs, zr, zx, zf = (per[i][key] for key in ("zs", "zr", "zx", "zf"))
        if k < p.mid:

            @pl.when(deep == k)
            def _():
                z_in(i, j).wait_recv()
                zs[j] = (zs[j].astype(F32) + zr[j].astype(F32)).astype(BF16)
                if k < p.mid - 1:
                    issue(functools.partial(z_in, i), j, SLOTS)
                else:
                    issue(functools.partial(z_cross, i), j, SLOTS)
        elif k == p.mid:

            @pl.when(deep == p.mid - 1)
            def _():
                z_cross(i, j).wait_recv()
                s = p.splits[i]
                own = xp[s.off : s.off + n * s.rb, columns_at(j)].astype(F32)
                zf[j] = (zs[j].astype(F32) + zx[j].astype(F32) + own).astype(BF16)
                if p.mid > 1:
                    issue(functools.partial(z_out, i), j, SLOTS)
                put(i, j)
        else:
            at = 2 * p.mid - 1 - k

            @pl.when(deep == at)
            def _():
                z_out(i, j).wait_recv()
                if at > 0:
                    issue(functools.partial(z_out, i), j, SLOTS)
                put(i, j)

    def shift(s, k):
        return [(first, last, start + k, pace) for first, last, start, pace in s.runs]

    def each(t, begin, end, runs, run):
        for first, last, start, pace in runs:
            for g in range(pace):
                stop = start - (g - (last - first)) // pace
                if begin >= stop or end <= start:
                    continue
                i = first + (t - start) * pace + g
                if start <= begin and end <= stop:
                    run(i)
                else:
                    pl.when((t >= start) & (t < stop))(functools.partial(run, i))

    def step(begin, end, t, carry):
        act_ = functools.partial(each, t, begin, end)
        if end <= C:
            up(t)
        if begin == 0:
            pl.semaphore_wait(barrier, nb + 1 + jnp.where(deep > 0, 1, 0))
        for i, s in enumerate(p.splits):
            act_([(0, J, s.down, 1)], functools.partial(down, i))
            act_(shift(s, 0), lambda c, i=i: issue(sum_copy(i, 0, 0), c, p.splits[i].send))
        for k in range(1, 2 * nb + 1):
            for i, s in enumerate(p.splits):
                if k < nb:
                    run = functools.partial(reduce, i, k)
                elif k == nb:
                    run = functools.partial(activate, i)
                elif k < 2 * nb:
                    run = functools.partial(gather, i, k - nb)
                else:
                    run = lambda c, i=i: act_copy(i, nb - 1, 0)(c).wait_recv()
                act_(shift(s, k), run)
        for k in range(1, 2 * p.mid):
            for i, s in enumerate(p.splits):
                act_([(0, J, s.down + p.after(s, k), 1)], functools.partial(z_step, i, k))
        return carry

    cuts = sorted(c for c in p.cuts if c < p.ticks) + [p.ticks]
    for begin, end in zip(cuts, cuts[1:]):
        if begin == C:
            for i in range(2):
                d_copy(0, i).start()
        if end == begin + 1:
            step(begin, end, begin, 0)
        else:
            lax.fori_loop(begin, end, functools.partial(step, begin, end), 0)

    for i in range(len(p.splits)):
        for c in range(max(C - p.splits[i].send, 0), C):
            sum_copy(i, 0, 0)(c).wait_send()
            act_copy(i, nb - 1, 0)(c).wait_send()
            for s in range(1, nb):
                sums_wait(i, s, c, "sk", p.splits[i].send)
            for k in range(nb - 1):
                acts_wait(i, k, c, "sa", p.splits[i].send)

        def finish(j, carry, i=i):
            z_in(i, j).wait_send()
            out_copy(i, j).wait()

            @pl.when(deep > 0)
            def _():
                z_out(i, j).wait_send()

            return carry

        lax.fori_loop(max(J - SLOTS, 0), J, finish, 0)


def body(n, nz, states, gc, gs, uc, us, dc, ds):
    rows, depth = states.shape
    hidden = gc.shape[1]
    p = Plan(n, nz, rows, depth, hidden)
    nb, C, J, wq = p.nb, p.c, p.j, p.wq
    dma = pltpu.SemaphoreType.DMA
    vmem = pl.BlockSpec(memory_space=pltpu.VMEM)
    hbm = pl.BlockSpec(memory_space=pl.ANY)
    two = (2,) * nb

    def own(s):
        item = pltpu.VMEM((J, n * s.rb, wq), BF16)
        return {
            "ps": pltpu.VMEM((C,) + two + (2, 2, s.rb, wq), BF16),
            "r0": pltpu.VMEM((C,) + two[1:] + (2, 2, s.rb, wq), BF16),
            "rk": [pltpu.VMEM((C, 2) + two[k + 1 :] + (2, s.rb, wq), BF16) for k in range(1, nb)],
            "act": pltpu.VMEM(two + (s.rb, hidden), BF16),
            "zs": item,
            "zr": item,
            "zx": item,
            "zf": item,
            "sem": {
                "s0": dma((s.send,)),
                "r0": dma((s.recv,)),
                "sk": dma((nb - 1, s.send)),
                "rk": dma((nb - 1, s.recv)),
                "sa": dma((nb - 1, s.send)),
                "ra": dma((nb - 1, s.recv)),
                "sl": dma((s.send,)),
                "rl": dma((s.recv,)),
                "zs": dma((SLOTS,)),
                "zr": dma((J,)),
                "zx": dma((J,)),
                "zo": dma((SLOTS,)),
                "zf": dma((J if p.mid > 2 else 1,)),
                "o": dma((SLOTS,)),
            },
        }

    out = pl.pallas_call(
        functools.partial(kernel, p),
        out_shape=jax.ShapeDtypeStruct((n, rows // n, depth), BF16),
        in_specs=[hbm] * 4 + [vmem] * 3,
        out_specs=hbm,
        scratch_shapes=[
            pltpu.VMEM((n, rows // n, depth), BF16),
            pltpu.VMEM((rows, depth), BF16),
            pltpu.VMEM((2, p.wrows, p.w), BF16),
            [own(s) for s in p.splits],
            {"x": dma((len(p.splits) * n,)), "w": dma((2, 2))},
        ],
        compiler_params=pltpu.CompilerParams(collective_id=0, has_side_effects=True, vmem_limit_bytes=67043328),
        cost_estimate=pl.CostEstimate(
            flops=6 * rows * depth * hidden, bytes_accessed=8 * depth * hidden, transcendentals=0
        ),
        name="mlp",
    )(states.reshape(n, rows // n, depth), gc, uc, dc, gs, us, ds)
    return out.reshape(rows, depth)


def solution(mesh):
    in_specs = (
        P(None, "mp"),
        P("mp", "hidden"),
        P("mp", "hidden"),
        P("mp", "hidden"),
        P("mp", "hidden"),
        P("hidden", "mp"),
        P("hidden", "mp"),
    )
    return jax.shard_map(
        functools.partial(body, mesh.shape["mp"], mesh.shape["hidden"]),
        mesh=mesh,
        in_specs=in_specs,
        out_specs=P(None, "mp"),
        check_vma=False,
    )
```

```python
import functools

import jax
import jax.numpy as jnp
from jax import lax
from jax.experimental import pallas as pl
from jax.experimental.pallas import tpu as pltpu
from jax.sharding import PartitionSpec as P

F32, BF16 = jnp.float32, jnp.bfloat16
MESH = pl.DeviceIdType.MESH
SLOTS = 4
SPLITS = ((2, 1, 1), (1, 1))
PACES = (1, 2, 2)
SLOW = (0, 3, 0)
LAGS = (4, 6, 7)


def dequant(codes, scales):
    depth, columns = codes.shape
    groups = scales.shape[0]
    blocks = codes.astype(F32).reshape(groups, depth // groups, columns)
    return (blocks * scales.reshape(groups, 1, columns)).reshape(depth, columns).astype(BF16)


class Split:
    def __init__(self, rb, row, off, runs, lag, pace):
        self.rb, self.row, self.off, self.runs, self.lag = rb, row, off, runs, lag
        self.send, self.recv = 2 * pace, 4 * pace


class Plan:
    def __init__(self, n, nz, rows, depth, hidden):
        self.n, self.nz, self.depth, self.hidden = n, nz, depth, hidden
        self.nb = n.bit_length() - 1
        self.rows = rows
        self.w = next(t for t in (512, 256) if hidden % t == 0)
        self.wq = self.w // 2
        self.c = hidden // self.w
        self.j = depth // self.wq
        self.k2 = hidden // 2
        self.wrows = max(2 * depth, self.k2)
        dims = list(range(self.nb))
        self.orders = (dims, dims[:1] + dims[:0:-1])
        self.mid = nz // 2
        rb = rows // n
        parts = next((p for p in SPLITS if all(rb * a % (16 * sum(p)) == 0 for a in p)), (1,))
        self.splits = []
        row, free, tick = 0, 0, 0
        for i, a in enumerate(parts):
            size = rb * a // sum(parts)
            pace = PACES[i] if i else 1
            slow = min(SLOW[i], self.c) if i else 0
            runs = []
            if slow:
                runs.append((0, slow, tick, 1))
                tick += slow
            if slow < self.c:
                runs.append((slow, self.c, tick, pace))
                tick += -(-(self.c - slow) // pace)
            split = Split(size, row, n * row, runs, LAGS[i], pace)
            split.down = max(tick + 2 * self.nb, free)
            free = split.down + self.j
            self.splits.append(split)
            row += size
        self.cuts = {0, 1, self.c} | {s.down for s in self.splits} | {s.down + self.j for s in self.splits}
        self.ticks = max(s.down + self.j - 1 + self.after(s, 2 * self.mid - 1) for s in self.splits) + 1

    def after(self, s, k):
        return -(-s.lag * k // 2)

    def left(self, q, k):
        return sorted(set(range(self.nb)) - set(self.orders[q][: k + 1]))

    def mask(self, pos):
        return sum(((pos >> (self.nb - 1 - d)) & 1) << d for d in range(self.nb))


def kernel(p, x_hbm, gc, uc, dc, gs, us, ds, out_hbm, out, xp, w, per, sems):
    n, nb, C, J, wq = p.n, p.nb, p.c, p.j, p.wq
    me = lax.axis_index("mp").astype(jnp.int32)
    z = lax.axis_index("hidden").astype(jnp.int32)
    nz = p.nz
    on_left = z < p.mid
    deep = jnp.where(on_left, z, nz - 1 - z)
    inward = jnp.where(on_left, z + 1, z - 1)
    outward = jnp.where(on_left, z - 1, z + 1)
    every = slice(None)

    def index(fixed, dims):
        return tuple(fixed.get(d, every) for d in dims)

    def columns_of(c):
        return pl.ds(pl.multiple_of(c * p.w, p.w), p.w)

    def columns_at(j):
        return pl.ds(pl.multiple_of(j * wq, wq), wq)

    def x_copy(i, pos):
        s = p.splits[i]
        return pltpu.make_async_copy(
            x_hbm.at[me ^ p.mask(pos), pl.ds(s.row, s.rb)],
            xp.at[pl.ds(s.off + pos * s.rb, s.rb)],
            sems["x"].at[i * n + pos],
        )

    def w_copy(c, i):
        slot = lax.rem(c, 3)
        return pltpu.make_async_copy(
            (gc, uc)[i].at[:, columns_of(c)], w.at[slot, pl.ds(i * p.depth, p.depth)], sems["w"].at[slot, i]
        )

    def d_copy(v, i):
        slot = lax.rem(v, 3)
        return pltpu.make_async_copy(
            dc.at[pl.ds(i * p.k2, p.k2), columns_at(lax.rem(v, J))],
            w.at[slot, pl.ds(0, p.k2), pl.ds(i * wq, wq)],
            sems["w"].at[slot, i],
        )

    def out_copy(i, j):
        s = p.splits[i]
        part = (every, pl.ds(s.row, s.rb), columns_at(j))
        return pltpu.make_async_copy(out.at[part], out_hbm.at[part], per[i]["sem"]["o"].at[lax.rem(j, SLOTS)])

    def remote(src, dst, send, recv, to):
        return pltpu.make_async_remote_copy(
            src_ref=src, dst_ref=dst, send_sem=send, recv_sem=recv, device_id=to, device_id_type=MESH
        )

    def part_at(c, q, fixed):
        return (c,) + index(fixed, range(nb)) + (q,)

    def sum_copy(i, s, q):
        d = p.orders[q][s]
        ps, r0, rk, sem = per[i]["ps"], per[i]["r0"], per[i]["rk"], per[i]["sem"]

        def make(c):
            slot, got = lax.rem(c, p.splits[i].send), lax.rem(c, p.splits[i].recv)
            to = (me ^ (1 << d), z)
            if s == 0:
                return remote(ps.at[c, 1], r0.at[c], sem["s0"].at[slot], sem["r0"].at[got], to)
            fixed = {e: 0 for e in p.orders[q][:s]} | {d: 1}
            return remote(
                ps.at[part_at(c, q, fixed)],
                rk[s - 1].at[c, q],
                sem["sk"].at[s - 1, slot],
                sem["rk"].at[s - 1, got],
                to,
            )

        return make

    def act_copy(i, k, q):
        d = p.orders[q][nb - 1 - k]
        whole = p.orders[q][nb - k :]
        act, sem = per[i]["act"], per[i]["sem"]

        def make(c):
            slot, got = lax.rem(c, p.splits[i].send), lax.rem(c, p.splits[i].recv)
            to = (me ^ (1 << d), z)
            last = k == nb - 1
            size = p.w if last else wq
            first = c * p.w + (0 if last else q * wq)
            columns = pl.ds(pl.multiple_of(first, wq), size)
            spots = [tuple(every if e in whole else (b if e == d else 0) for e in range(nb)) for b in (0, 1)]
            src, dst = (act.at[spot + (every, columns)] for spot in spots)
            if last:
                return remote(src, dst, sem["sl"].at[slot], sem["rl"].at[got], to)
            return remote(src, dst, sem["sa"].at[k, slot], sem["ra"].at[k, got], to)

        return make

    def issue(make, c, slots):
        @pl.when(c >= slots)
        def _():
            make(c - slots).wait_send()

        make(c).start()

    def sums_wait(i, s, c, key, slots):
        both = per[i]["rk"][s - 1].at[c]
        pltpu.make_async_copy(both, both, per[i]["sem"][key].at[s - 1, lax.rem(c, slots)]).wait()

    def acts_wait(i, k, c, key, slots):
        both = per[i]["act"].at[(0,) * (nb - k) + (every,) * k + (every, columns_of(c))]
        pltpu.make_async_copy(both, both, per[i]["sem"][key].at[k, lax.rem(c, slots)]).wait()

    def make_room(wait, i, k, c, key):
        slots = p.splits[i].send

        @pl.when(c >= slots)
        def _():
            wait(i, k, c - slots, key, slots)

    for i in range(len(p.splits)):
        for pos in range(n):
            x_copy(i, pos).start()
    for i in range(2):
        w_copy(0, i).start()
    barrier = pltpu.get_barrier_semaphore()
    for d in range(nb):
        pl.semaphore_signal(barrier, inc=1, device_id=(me ^ (1 << d), z), device_id_type=MESH)
    pl.semaphore_signal(barrier, inc=1, device_id=(me, inward), device_id_type=MESH)

    @pl.when(deep > 0)
    def _():
        pl.semaphore_signal(barrier, inc=1, device_id=(me, outward), device_id_type=MESH)

    for i in range(len(p.splits)):
        for pos in range(n):
            x_copy(i, pos).wait()

    def up(c):
        @pl.when(c + 1 < C)
        def _():
            for i in range(2):
                w_copy(c + 1, i).start()

        slot = lax.rem(c, 3)
        for i, scales in enumerate((gs, us)):
            w_copy(c, i).wait()
            weight = dequant(w[slot, i * p.depth : (i + 1) * p.depth], scales[:, columns_of(c)])
            part = jnp.dot(xp[...], weight, preferred_element_type=F32).astype(BF16)
            for s, own in zip(p.splits, per):
                rows = part[s.off : s.off + n * s.rb].reshape((2,) * nb + (s.rb, p.w))
                for q in range(2):
                    own["ps"][(c,) + (every,) * nb + (q, i)] = rows[..., q * wq : (q + 1) * wq]

    def total(own, c, q, fixed, count):
        value = own["ps"][part_at(c, q, fixed)].astype(F32)
        if count > 0:
            value = value + own["r0"][(c,) + index(fixed, range(1, nb)) + (q,)].astype(F32)
        for k in range(1, count):
            value = value + own["rk"][k - 1][(c, q) + index(fixed, p.left(q, k))].astype(F32)
        return value

    def reduce(i, s, c):
        if s == 1:
            sum_copy(i, 0, 0)(c).wait_recv()
        else:
            sums_wait(i, s - 1, c, "rk", p.splits[i].recv)
        make_room(sums_wait, i, s, c, "sk")
        for q in range(2):
            fixed = {e: 0 for e in p.orders[q][:s]} | {p.orders[q][s]: 1}
            per[i]["ps"][part_at(c, q, fixed)] = total(per[i], c, q, fixed, s).astype(BF16)
            sum_copy(i, s, q)(c).start()

    def activate(i, c):
        sums_wait(i, nb - 1, c, "rk", p.splits[i].recv)
        make_room(acts_wait, i, 0, c, "sa")
        for q in range(2):
            both = total(per[i], c, q, {e: 0 for e in range(nb)}, nb)
            gate, up_ = both[0], both[1]
            columns = pl.ds(pl.multiple_of(c * p.w + q * wq, wq), wq)
            per[i]["act"][(0,) * nb + (every, columns)] = (gate / (1.0 + jnp.exp(-gate)) * up_).astype(BF16)
            act_copy(i, 0, q)(c).start()

    def gather(i, k, c):
        acts_wait(i, k - 1, c, "ra", p.splits[i].recv)
        if k < nb - 1:
            make_room(acts_wait, i, k, c, "sa")
            for q in range(2):
                act_copy(i, k, q)(c).start()
        else:
            issue(act_copy(i, k, 0), c, p.splits[i].send)

    def down(i, j):
        v = i * J + j

        @pl.when(v + 2 < J * len(p.splits))
        def _():
            for k in range(2):
                d_copy(v + 2, k).start()

        own = per[i]
        slot = lax.rem(v, 3)
        groups = ds.shape[0] // 2
        value = None
        for k in range(2):
            d_copy(v, k).wait()
            weight = dequant(
                w[slot, : p.k2, k * wq : (k + 1) * wq], ds[k * groups : (k + 1) * groups, columns_at(j)]
            )
            a = own["act"][(every,) * nb + (every, slice(k * p.k2, (k + 1) * p.k2))]
            term = jnp.dot(a.reshape(n * p.splits[i].rb, p.k2), weight, preferred_element_type=F32)
            value = term if value is None else value + term
        own["zs"][j] = value.astype(BF16)

        @pl.when(deep == 0)
        def _():
            issue(functools.partial(z_in, i), j, SLOTS)

    def z_in(i, j):
        own, sem = per[i], per[i]["sem"]
        return remote(own["zs"].at[j], own["zr"].at[j], sem["zs"].at[lax.rem(j, SLOTS)], sem["zr"].at[j], (me, inward))

    def z_cross(i, j):
        own, sem = per[i], per[i]["sem"]
        return remote(own["zs"].at[j], own["zx"].at[j], sem["zs"].at[lax.rem(j, SLOTS)], sem["zx"].at[j], (me, inward))

    def z_out(i, j):
        own, sem = per[i], per[i]["sem"]
        return remote(own["zf"].at[j], own["zf"].at[j], sem["zo"].at[lax.rem(j, SLOTS)], sem["zf" if p.mid > 2 else "zr"].at[j], (me, outward))

    def put(i, j):
        s = p.splits[i]
        for pos in range(n):
            out[me ^ p.mask(pos), s.row : s.row + s.rb, columns_at(j)] = per[i]["zf"][j, pos * s.rb : (pos + 1) * s.rb]

        @pl.when(j >= SLOTS)
        def _():
            out_copy(i, j - SLOTS).wait()

        out_copy(i, j).start()

    def z_step(i, k, j):
        zs, zr, zx, zf = (per[i][key] for key in ("zs", "zr", "zx", "zf"))
        if k < p.mid:

            @pl.when(deep == k)
            def _():
                z_in(i, j).wait_recv()
                zs[j] = (zs[j].astype(F32) + zr[j].astype(F32)).astype(BF16)
                if k < p.mid - 1:
                    issue(functools.partial(z_in, i), j, SLOTS)
                else:
                    issue(functools.partial(z_cross, i), j, SLOTS)
        elif k == p.mid:

            @pl.when(deep == p.mid - 1)
            def _():
                z_cross(i, j).wait_recv()
                s = p.splits[i]
                own = xp[s.off : s.off + n * s.rb, columns_at(j)].astype(F32)
                zf[j] = (zs[j].astype(F32) + zx[j].astype(F32) + own).astype(BF16)
                if p.mid > 1:
                    issue(functools.partial(z_out, i), j, SLOTS)
                put(i, j)
        else:
            at = 2 * p.mid - 1 - k

            @pl.when(deep == at)
            def _():
                z_out(i, j).wait_recv()
                if at > 0:
                    issue(functools.partial(z_out, i), j, SLOTS)
                put(i, j)

    def shift(s, k):
        return [(first, last, start + k, pace) for first, last, start, pace in s.runs]

    def each(t, begin, end, runs, run):
        for first, last, start, pace in runs:
            for g in range(pace):
                stop = start - (g - (last - first)) // pace
                if begin >= stop or end <= start:
                    continue
                i = first + (t - start) * pace + g
                if start <= begin and end <= stop:
                    run(i)
                else:
                    pl.when((t >= start) & (t < stop))(functools.partial(run, i))

    def step(begin, end, t, carry):
        act_ = functools.partial(each, t, begin, end)
        if end <= C:
            up(t)
        if begin == 0:
            pl.semaphore_wait(barrier, nb + 1 + jnp.where(deep > 0, 1, 0))
        for i, s in enumerate(p.splits):
            act_([(0, J, s.down, 1)], functools.partial(down, i))
            act_(shift(s, 0), lambda c, i=i: issue(sum_copy(i, 0, 0), c, p.splits[i].send))
        for k in range(1, 2 * nb + 1):
            for i, s in enumerate(p.splits):
                if k < nb:
                    run = functools.partial(reduce, i, k)
                elif k == nb:
                    run = functools.partial(activate, i)
                elif k < 2 * nb:
                    run = functools.partial(gather, i, k - nb)
                else:
                    run = lambda c, i=i: act_copy(i, nb - 1, 0)(c).wait_recv()
                act_(shift(s, k), run)
        for k in range(1, 2 * p.mid):
            for i, s in enumerate(p.splits):
                act_([(0, J, s.down + p.after(s, k), 1)], functools.partial(z_step, i, k))
        return carry

    cuts = sorted(c for c in p.cuts if c < p.ticks) + [p.ticks]
    for begin, end in zip(cuts, cuts[1:]):
        if begin == C:
            for v in range(2):
                for i in range(2):
                    d_copy(v, i).start()
        if end == begin + 1:
            step(begin, end, begin, 0)
        else:
            lax.fori_loop(begin, end, functools.partial(step, begin, end), 0)

    for i in range(len(p.splits)):
        for c in range(max(C - p.splits[i].send, 0), C):
            sum_copy(i, 0, 0)(c).wait_send()
            act_copy(i, nb - 1, 0)(c).wait_send()
            for s in range(1, nb):
                sums_wait(i, s, c, "sk", p.splits[i].send)
            for k in range(nb - 1):
                acts_wait(i, k, c, "sa", p.splits[i].send)

        def finish(j, carry, i=i):
            z_in(i, j).wait_send()
            out_copy(i, j).wait()

            @pl.when(deep > 0)
            def _():
                z_out(i, j).wait_send()

            return carry

        lax.fori_loop(max(J - SLOTS, 0), J, finish, 0)


def body(n, nz, states, gc, gs, uc, us, dc, ds):
    rows, depth = states.shape
    hidden = gc.shape[1]
    p = Plan(n, nz, rows, depth, hidden)
    nb, C, J, wq = p.nb, p.c, p.j, p.wq
    dma = pltpu.SemaphoreType.DMA
    vmem = pl.BlockSpec(memory_space=pltpu.VMEM)
    hbm = pl.BlockSpec(memory_space=pl.ANY)
    two = (2,) * nb

    def own(s):
        item = pltpu.VMEM((J, n * s.rb, wq), BF16)
        return {
            "ps": pltpu.VMEM((C,) + two + (2, 2, s.rb, wq), BF16),
            "r0": pltpu.VMEM((C,) + two[1:] + (2, 2, s.rb, wq), BF16),
            "rk": [pltpu.VMEM((C, 2) + two[k + 1 :] + (2, s.rb, wq), BF16) for k in range(1, nb)],
            "act": pltpu.VMEM(two + (s.rb, hidden), BF16),
            "zs": item,
            "zr": item,
            "zx": item,
            "zf": item,
            "sem": {
                "s0": dma((s.send,)),
                "r0": dma((s.recv,)),
                "sk": dma((nb - 1, s.send)),
                "rk": dma((nb - 1, s.recv)),
                "sa": dma((nb - 1, s.send)),
                "ra": dma((nb - 1, s.recv)),
                "sl": dma((s.send,)),
                "rl": dma((s.recv,)),
                "zs": dma((SLOTS,)),
                "zr": dma((J,)),
                "zx": dma((J,)),
                "zo": dma((SLOTS,)),
                "zf": dma((J if p.mid > 2 else 1,)),
                "o": dma((SLOTS,)),
            },
        }

    out = pl.pallas_call(
        functools.partial(kernel, p),
        out_shape=jax.ShapeDtypeStruct((n, rows // n, depth), BF16),
        in_specs=[hbm] * 4 + [vmem] * 3,
        out_specs=hbm,
        scratch_shapes=[
            pltpu.VMEM((n, rows // n, depth), BF16),
            pltpu.VMEM((rows, depth), BF16),
            pltpu.VMEM((3, p.wrows, p.w), BF16),
            [own(s) for s in p.splits],
            {"x": dma((len(p.splits) * n,)), "w": dma((3, 2))},
        ],
        compiler_params=pltpu.CompilerParams(collective_id=0, has_side_effects=True, vmem_limit_bytes=67043328),
        cost_estimate=pl.CostEstimate(
            flops=6 * rows * depth * hidden, bytes_accessed=8 * depth * hidden, transcendentals=0
        ),
        name="mlp",
    )(states.reshape(n, rows // n, depth), gc, uc, dc, gs, us, ds)
    return out.reshape(rows, depth)


def solution(mesh):
    in_specs = (
        P(None, "mp"),
        P("mp", "hidden"),
        P("mp", "hidden"),
        P("mp", "hidden"),
        P("mp", "hidden"),
        P("hidden", "mp"),
        P("hidden", "mp"),
    )
    return jax.shard_map(
        functools.partial(body, mesh.shape["mp"], mesh.shape["hidden"]),
        mesh=mesh,
        in_specs=in_specs,
        out_specs=P(None, "mp"),
        check_vma=False,
    )
```
